32 devices in a mesh: rep: 2 (over x), dp: 16 (over y, z, core).
Axes of the slice: x: 2, y: 2, z: 4, core: 2. Of those that a mesh axis runs over, the one named last changes fastest.
Arguments:
- x: bfloat16 [32, 2048, 896], P(('rep', 'dp')), parts along dimension 0
- dy: bfloat16 [32, 2048, 896], P(('rep', 'dp')), parts along dimension 0
- w_gate: bfloat16 [2, 896, 2560], P(None, 'dp')
- w_up: bfloat16 [2, 896, 2560], P(None, 'dp')
- w_down: bfloat16 [2, 2560, 896], P(None, 'dp')
Outputs:
- output 1: bfloat16 [32, 2048, 896], P(('rep', 'dp')), parts along dimension 0
- output 2: bfloat16 [4, 896, 2560], P('rep', 'dp'), parts along dimension 0
- output 3: bfloat16 [4, 896, 2560], P('rep', 'dp'), parts along dimension 0
- output 4: bfloat16 [4, 2560, 896], P('rep', 'dp'), parts along dimension 0
There are 2 independent parts. The reference program is written for one: setup_inputs(seed, part) draws one part's arguments, and reference() takes and returns one part's arrays. A program takes and returns all parts, laid end to end along the dimension named above; an argument that names none is the same for every part.
All inputs are finite; a program needn't handle non-finite values.
Results may differ from the reference program's by a relative error of at most 0.018.
Values are sent between devices in bfloat16 or wider.
A program may use at most 2 GiB of HBM per device.

```python
import jax
import jax.numpy as jnp
from jax import lax

SEQUENCES = 16
TOKENS = 2048
D = 896
FF = 2560
LAYERS = 2
NAMES = ("w_gate", "w_up", "w_down")
SHAPES = {"w_gate": (LAYERS, D, FF), "w_up": (LAYERS, D, FF), "w_down": (LAYERS, FF, D)}


def bump(key, n, height):
    away = (jnp.arange(n, dtype=jnp.int32) - jax.random.randint(key, (), 0, n, jnp.int32)) % n
    return jnp.where(away < n // 8, height, 1.0)


def together(key, own, strength):
    shared = jax.random.normal(key, own.shape[1:], jnp.float32)
    return (own + strength * shared) * lax.rsqrt(1 + strength * strength)


def setup_inputs(seed: int = 0, part: int = 0) -> dict:
    kx, kdy, ka, kb, kz, kf, kh, kl, *kw = jax.random.split(jax.random.key(seed), 8 + len(NAMES))
    kx, kdy, ka, kb = (jax.random.fold_in(k, part) for k in (kx, kdy, ka, kb))
    shape = (SEQUENCES, TOKENS, D)
    much_x, much_dy = jax.random.uniform(kz, (2,), jnp.float32, 0.0, 1.0)
    layers = 2.0 ** jax.random.uniform(kl, (LAYERS, 1, 1), jnp.float32, -1.0, 1.0)
    x = together(ka, jax.random.normal(kx, shape, jnp.float32), much_x) * bump(kf, D, 4.0)
    dy = together(kb, jax.random.normal(kdy, shape, jnp.float32), much_dy)
    drawn = {"x": x.astype(jnp.bfloat16), "dy": (dy * (SEQUENCES * TOKENS) ** -0.5).astype(jnp.bfloat16)}
    for key, name in zip(kw, NAMES, strict=True):
        w = jax.random.normal(key, SHAPES[name], jnp.float32) * SHAPES[name][1] ** -0.5
        drawn[name] = (w * {"w_gate": 1.0, "w_up": bump(kh, FF, 4.0), "w_down": layers}[name]).astype(jnp.bfloat16)
    return drawn


def matmul(a, w):
    return jnp.dot(a, w, preferred_element_type=jnp.float32).astype(jnp.bfloat16)


def normed(h):
    wide = h.astype(jnp.float32)
    scale = lax.rsqrt(jnp.mean(wide**2, -1, keepdims=True) + 1e-6)
    return (wide * scale).astype(jnp.bfloat16)


def layer(h, w):
    a = normed(h)
    gate = jnp.dot(a, w["w_gate"], preferred_element_type=jnp.float32)
    up = jnp.dot(a, w["w_up"], preferred_element_type=jnp.float32)
    return h + matmul((jax.nn.silu(gate) * up).astype(jnp.bfloat16), w["w_down"])


def stack(weights, h):
    return lax.scan(lambda h, w: (layer(h, w), None), h, weights)[0]


def reference(x, dy, w_gate, w_up, w_down):
    weights = dict(zip(NAMES, (w_gate, w_up, w_down), strict=True))

    def take(so_far, sequence):
        h, by_y = sequence
        _, back = jax.vjp(stack, weights, h)
        by_weights, by_h = back(by_y)
        return jax.tree.map(lambda total, term: total + term.astype(jnp.float32), so_far, by_weights), by_h

    none_yet = {name: jnp.zeros(w.shape, jnp.float32) for name, w in weights.items()}
    by_weights, by_x = lax.scan(take, none_yet, (x, dy))
    return (by_x, *(by_weights[name].astype(jnp.bfloat16) for name in NAMES))
```

```python
import functools

import jax
import jax.numpy as jnp
from jax import lax
from jax.experimental import pallas as pl
from jax.experimental.pallas import tpu as pltpu
from jax.sharding import PartitionSpec as P

BF16, F32 = jnp.bfloat16, jnp.float32
ANY = pl.BlockSpec(memory_space=pl.ANY)
VMEM_LIMIT = 62 * 1024 * 1024
NY, NZ = 2, 4
TOKENS, CHUNK = 512, 512


def device(y, z, c):
    return (y * NZ + z) * 2 + c


class Place:
    def __init__(self):
        self.me = lax.axis_index("dp")
        self.c = lax.rem(self.me, 2)
        self.z = lax.rem(lax.div(self.me, 2), NZ)
        self.y = lax.div(self.me, 2 * NZ)
        self.y_mate = device(1 - self.y, self.z, self.c)
        self.sibling = device(self.y, self.z, 1 - self.c)

    def ahead(self, d):
        return lax.rem(self.z + d, NZ)

    def behind(self, d):
        return lax.rem(self.z + NZ - d, NZ)

    def z_mate(self, d):
        return device(self.y, self.ahead(d), self.c)

    def greet(self):
        barrier = pltpu.get_barrier_semaphore()
        mates = [self.z_mate(d) for d in (1, 2, 3)] + [self.y_mate, self.sibling]
        for mate in mates:
            pl.semaphore_signal(barrier, inc=1, device_id={"dp": mate}, device_id_type=pl.DeviceIdType.MESH)
        pl.semaphore_wait(barrier, len(mates))


def remote(src, dst, send, recv, to):
    return pltpu.make_async_remote_copy(
        src_ref=src, dst_ref=dst, send_sem=send, recv_sem=recv, device_id={"dp": to}, device_id_type=pl.DeviceIdType.MESH
    )


class Gather:
    def __init__(self, place, src, out, stage, send, recv, local):
        self.p, self.src, self.out, self.stage, self.send, self.recv, self.local = place, src, out, stage, send, recv, local
        self.rows = src.shape[0]

    def block(self, j):
        return self.out.at[pl.ds(pl.multiple_of(j * self.rows, 8), self.rows), :]

    def copy(self, src, dst, slot, to):
        return remote(src, dst, self.send.at[slot], self.recv.at[slot], to)

    def begin(self):
        p, mine = self.p, self.block(self.p.me)
        for d in (1, 2, 3):
            self.copy(self.src, mine, d - 1, p.z_mate(d)).start()
        self.copy(self.src, mine, 3, p.y_mate).start()
        self.copy(self.src, mine, 7, p.sibling).start()
        own = pltpu.make_async_copy(self.src, self.stage, self.local.at[0])
        own.start()
        own.wait()
        pltpu.make_async_copy(self.stage, mine, self.local.at[1]).start()

    def from_z(self, d):
        p = self.p
        block = self.block(device(p.y, p.behind(d), p.c))
        self.copy(block, block, d - 1, p.y_mate).wait_recv()
        self.copy(block, block, 3 + d, p.y_mate).start()
        self.copy(block, block, 7 + d, p.sibling).start()

    def from_y(self, d):
        p = self.p
        block = self.block(device(1 - p.y, p.behind(d), p.c))
        self.copy(block, block, 3 + d, p.y_mate).wait_recv()
        self.copy(block, block, 11 + d, p.sibling).start()

    def finish(self):
        p = self.p
        for k in range(8):
            row = p.y if k < 4 else 1 - p.y
            block = self.block(device(row, p.behind(k % 4), 1 - p.c))
            self.copy(block, block, 7 + k, p.sibling).wait_recv()
        mine = self.block(p.me)
        for slot in range(15):
            self.copy(mine, mine, slot, p.sibling).wait_send()
        pltpu.make_async_copy(self.stage, mine, self.local.at[1]).wait()

    @staticmethod
    def scratch(shape):
        return [pltpu.VMEM(shape, BF16), pltpu.SemaphoreType.DMA((15,)), pltpu.SemaphoreType.DMA((15,)), pltpu.SemaphoreType.DMA((2,))]


class Scatter:
    def __init__(self, place, src, out, own, sib, from_y, from_z, total, send, recv, local):
        self.p, self.src, self.out, self.total = place, src, out, total
        self.own, self.sib, self.y_slots, self.z_slots = own, sib, from_y, from_z
        self.send, self.recv, self.local = send, recv, local
        self.rows = out.shape[0]

    def block(self, k, c):
        row = 1 - self.p.y if k < 4 else self.p.y
        j = device(row, self.p.ahead(k % 4), c)
        return self.src.at[pl.ds(pl.multiple_of(j * self.rows, 8), self.rows), :]

    def to_sibling(self, k):
        return remote(self.block(k, 1 - self.p.c), self.sib.at[k], self.send.at[k], self.recv.at[k], self.p.sibling)

    def to_y(self, d):
        return remote(self.own.at[d], self.y_slots.at[d], self.send.at[8 + d], self.recv.at[8 + d], self.p.y_mate)

    def to_z(self, d):
        return remote(self.own.at[4 + d], self.z_slots.at[d - 1], self.send.at[11 + d], self.recv.at[11 + d], self.p.z_mate(d))

    def load(self, k):
        return pltpu.make_async_copy(self.block(k, self.p.c), self.own.at[k], self.local.at[k])

    def begin(self):
        for k in (1, 2, 3, 0, 5, 6, 7, 4):
            self.to_sibling(k).start()
            self.load(k).start()

    def add(self, refs, to):
        rows, columns = self.rows, self.own.shape[2]
        if columns % 512 == 0:
            count, at = columns // 256, lambda i: (slice(None), pl.ds(pl.multiple_of(i * 256, 256), 256))
        else:
            count, at = rows // 16, lambda i: (pl.ds(pl.multiple_of(i * 16, 16), 16), slice(None))

        def some(i, carry):
            here = at(i)
            value = refs[0][here].astype(F32)
            for ref in refs[1:]:
                value = value + ref[here].astype(F32)
            to[here] = value.astype(BF16)
            return carry

        lax.fori_loop(0, count, some, 0)

    def send_y(self, d):
        self.load(d).wait()
        self.to_sibling(d).wait_recv()
        self.add((self.own.at[d], self.sib.at[d]), self.own.at[d])
        self.to_y(d).start()

    def send_z(self, d):
        self.load(4 + d).wait()
        self.to_sibling(4 + d).wait_recv()
        self.to_y(d).wait_recv()
        self.add((self.own.at[4 + d], self.sib.at[4 + d], self.y_slots.at[d]), self.own.at[4 + d])
        self.to_z(d).start()

    def finish(self):
        self.load(4).wait()
        self.to_sibling(4).wait_recv()
        self.to_y(0).wait_recv()
        for d in (1, 2, 3):
            self.to_z(d).wait_recv()
        self.add([self.own.at[4], self.sib.at[4], self.y_slots.at[0]] + [self.z_slots.at[d] for d in range(3)], self.total)
        store = pltpu.make_async_copy(self.total, self.out, self.local.at[8])
        store.start()
        for k in range(8):
            self.to_sibling(k).wait_send()
        for d in range(4):
            self.to_y(d).wait_send()
        for d in (1, 2, 3):
            self.to_z(d).wait_send()
        store.wait()

    @staticmethod
    def scratch(shape):
        return [pltpu.VMEM((n, *shape), BF16) for n in (8, 8, 4, 3)] + [
            pltpu.VMEM(shape, BF16),
            pltpu.SemaphoreType.DMA((15,)),
            pltpu.SemaphoreType.DMA((15,)),
            pltpu.SemaphoreType.DMA((9,)),
        ]


def gather_events(jobs):
    events = []
    for n in range(len(jobs) + 1):
        if n < len(jobs):
            events += [functools.partial(jobs[n].from_z, d) for d in (1, 2, 3)]
        if n > 0:
            events += [functools.partial(jobs[n - 1].from_y, d) for d in (0, 1, 2, 3)]
    return events + [job.finish for job in jobs]


def scatter_events(jobs):
    events = []
    for n in range(len(jobs) + 2):
        if n < len(jobs):
            events += [functools.partial(jobs[n].send_y, d) for d in (1, 2, 3, 0)]
        if 0 < n <= len(jobs):
            events += [functools.partial(jobs[n - 1].send_z, d) for d in (1, 2, 3)]
        if n > 1:
            events.append(jobs[n - 2].finish)
    return events


def spread(events, steps):
    by_step = [[] for _ in range(steps)]
    for n, event in enumerate(events):
        by_step[n * steps // len(events)].append(event)
    return by_step


def at_step(by_step, step):
    for n, events in enumerate(by_step):
        if events:

            @pl.when(step == n)
            def _(events=events):
                for event in events:
                    event()


def dot(a, b, contract):
    return lax.dot_general(a, b, (contract, ((), ())), preferred_element_type=F32)


def scale_of(wide):
    return lax.rsqrt(jnp.mean(wide * wide, -1, keepdims=True) + 1e-6)


def forward(h, wg, wu, wd, out, a, acc, hook):
    tokens, dim = h.shape
    tiles, chunks = tokens // TOKENS, wg.shape[1] // CHUNK

    def body(h, wg, wu, wd, out):
        t, f = pl.program_id(0), pl.program_id(1)
        hook(t * chunks + f)

        @pl.when(f == 0)
        def _():
            wide = h[...].astype(F32)
            a[...] = (wide * scale_of(wide)).astype(BF16)
            acc[...] = jnp.zeros_like(acc)

        gate = dot(a[...], wg[...], ((1,), (0,)))
        up = dot(a[...], wu[...], ((1,), (0,)))
        hid = (gate * jax.nn.sigmoid(gate) * up).astype(BF16)
        acc[...] += dot(hid, wd[...], ((1,), (0,)))

        @pl.when(f == chunks - 1)
        def _():
            out[...] = (h[...].astype(F32) + acc[...].astype(BF16).astype(F32)).astype(BF16)

    whole = pl.BlockSpec((TOKENS, dim), lambda t, f: (t, 0))
    pltpu.emit_pipeline(
        body,
        grid=(tiles, chunks),
        in_specs=[
            whole,
            pl.BlockSpec((dim, CHUNK), lambda t, f: (0, f)),
            pl.BlockSpec((dim, CHUNK), lambda t, f: (0, f)),
            pl.BlockSpec((CHUNK, dim), lambda t, f: (f, 0)),
        ],
        out_specs=[whole],
    )(h, wg, wu, wd, out)


def backward(h, dy, wg, wu, wd, dh, a, hid, dgate, dup, acc, hook):
    tokens, dim = h.shape
    tiles, chunks = tokens // TOKENS, wg.shape[1] // CHUNK

    def body(h, dy, wg, wu, wd, dh, a, hid, dgate, dup):
        t, f = pl.program_id(0), pl.program_id(1)
        hook(t * chunks + f)

        @pl.when(f == 0)
        def _():
            wide = h[...].astype(F32)
            a[...] = (wide * scale_of(wide)).astype(BF16)
            acc[...] = jnp.zeros_like(acc)

        gate = dot(a[...], wg[...], ((1,), (0,)))
        up = dot(a[...], wu[...], ((1,), (0,)))
        dhid = dot(dy[...], wd[...], ((1,), (1,))).astype(BF16).astype(F32)
        s = jax.nn.sigmoid(gate)
        silu = gate * s
        hid[...] = (silu * up).astype(BF16)
        by_gate = (dhid * up * (s * (1 + gate * (1 - s)))).astype(BF16)
        by_up = (dhid * silu).astype(BF16)
        dgate[...] = by_gate
        dup[...] = by_up
        acc[...] += dot(by_gate, wg[...], ((1,), (1,))) + dot(by_up, wu[...], ((1,), (1,)))

        @pl.when(f == chunks - 1)
        def _():
            wide = h[...].astype(F32)
            scale = scale_of(wide)
            da = acc[...].astype(BF16).astype(F32)
            along = jnp.mean(da * wide, -1, keepdims=True)
            by_h = (da * scale - wide * (along * scale * scale * scale)).astype(BF16)
            dh[...] = (dy[...].astype(F32) + by_h.astype(F32)).astype(BF16)

    whole = pl.BlockSpec((TOKENS, dim), lambda t, f: (t, 0))
    part = pl.BlockSpec((TOKENS, CHUNK), lambda t, f: (t, f))
    pltpu.emit_pipeline(
        body,
        grid=(tiles, chunks),
        in_specs=[
            whole,
            whole,
            pl.BlockSpec((dim, CHUNK), lambda t, f: (0, f)),
            pl.BlockSpec((dim, CHUNK), lambda t, f: (0, f)),
            pl.BlockSpec((CHUNK, dim), lambda t, f: (f, 0)),
        ],
        out_specs=[whole, whole, part, part, part],
    )(h, dy, wg, wu, wd, dh, a, hid, dgate, dup)


def by_weights(a, dy, hid, dgate, dup, dwg, dwu, dwd, hook):
    tokens, dim = a.shape
    chunks = hid.shape[1] // CHUNK

    def body(a, dy, hid, dgate, dup, dwg, dwu, dwd):
        hook(pl.program_id(0))
        dwd[...] = dot(hid[...], dy[...], ((0,), (0,))).astype(BF16)
        dwg[...] = dot(a[...], dgate[...], ((0,), (0,))).astype(BF16)
        dwu[...] = dot(a[...], dup[...], ((0,), (0,))).astype(BF16)

    whole = pl.BlockSpec((tokens, dim), lambda f: (0, 0))
    part = pl.BlockSpec((tokens, CHUNK), lambda f: (0, f))
    wide = pl.BlockSpec((dim, CHUNK), lambda f: (0, f))
    pltpu.emit_pipeline(
        body,
        grid=(chunks,),
        in_specs=[whole, whole, part, part, part],
        out_specs=[wide, wide, pl.BlockSpec((CHUNK, dim), lambda f: (f, 0))],
    )(a, dy, hid, dgate, dup, dwg, dwu, dwd)


def nothing(step):
    pass


def call(body, outs, scratch, collective, *args):
    return pl.pallas_call(
        body,
        out_shape=[jax.ShapeDtypeStruct(shape, BF16) for shape in outs],
        in_specs=[ANY] * len(args),
        out_specs=[ANY] * len(outs),
        scratch_shapes=scratch,
        compiler_params=pltpu.CompilerParams(collective_id=collective, has_side_effects=True, vmem_limit_bytes=VMEM_LIMIT)
        if collective is not None
        else pltpu.CompilerParams(vmem_limit_bytes=VMEM_LIMIT),
    )(*args)


def solution(mesh):
    def step(x, dy, *weights):
        tokens, dim = x.shape[1:]
        ff = weights[0].shape[2]
        x, dy = x[0], dy[0]
        shards = [w.shape[1:] for w in weights]
        wholes = [(16 * r, c) for r, c in shards]
        n_gather, n_scatter = len(Gather.scratch((8, 128))), len(Scatter.scratch((8, 128)))
        gather_scratch = [s for shape in shards for s in Gather.scratch(shape)]
        scatter_scratch = [s for shape in shards for s in Scatter.scratch(shape)]

        def gathers(n, place, srcs, outs, scratch):
            return [Gather(place, srcs[i].at[n], outs[i], *scratch[n_gather * i : n_gather * (i + 1)]) for i in range(3)]

        def scatters(place, srcs, outs, scratch):
            return [Scatter(place, srcs[i], outs[i], *scratch[n_scatter * i : n_scatter * (i + 1)]) for i in range(3)]

        def k1(*refs):
            place = Place()
            place.greet()
            jobs = gathers(0, place, refs[:3], refs[3:6], refs[6:])
            for job in jobs:
                job.begin()
            for event in gather_events(jobs):
                event()

        first = call(k1, wholes, gather_scratch, 1, *weights)

        def k2(*refs):
            h, wg, wu, wd = refs[:4]
            place = Place()
            place.greet()
            out = refs[7]
            jobs = gathers(1, place, refs[4:7], refs[8:11], refs[13:])
            for job in jobs:
                job.begin()
            steps = (tokens // TOKENS) * (ff // CHUNK)
            by_step = spread(gather_events(jobs), steps)
            forward(h, wg, wu, wd, out, refs[11], refs[12], functools.partial(at_step, by_step))

        tile = [pltpu.VMEM((TOKENS, dim), BF16), pltpu.VMEM((TOKENS, dim), F32)]
        h1, *second = call(k2, [(tokens, dim), *wholes], tile + gather_scratch, 2, x, *first, *weights)

        acc = [pltpu.VMEM((TOKENS, dim), F32)]
        saved = [(tokens, dim), (tokens, dim), (tokens, ff), (tokens, ff), (tokens, ff)]

        def k3(*refs):
            h, dy, wg, wu, wd, dh, a, hid, dgate, dup, dwg, dwu, dwd, acc = refs
            backward(h, dy, wg, wu, wd, dh, a, hid, dgate, dup, acc, nothing)
            by_weights(a, dy, hid, dgate, dup, dwg, dwu, dwd, nothing)

        d1, _, _, _, _, *terms1 = call(k3, saved + wholes, acc, None, h1, dy, *second)

        def k4(*refs):
            h, dy, wg, wu, wd = refs[:5]
            terms = refs[5:8]
            dh, a, hid, dgate, dup, dwg, dwu, dwd = refs[8:16]
            outs = refs[16:19]
            acc = refs[19]
            place = Place()
            place.greet()
            jobs = scatters(place, terms, outs, refs[20:])
            for job in jobs:
                job.begin()
            steps = (tokens // TOKENS) * (ff // CHUNK)
            by_step = spread(scatter_events(jobs), steps + 5)
            backward(h, dy, wg, wu, wd, dh, a, hid, dgate, dup, acc, functools.partial(at_step, by_step[:steps]))
            by_weights(a, dy, hid, dgate, dup, dwg, dwu, dwd, functools.partial(at_step, by_step[steps:]))

        d0, _, _, _, _, *rest = call(k4, saved + wholes + shards, acc + scatter_scratch, 3, x, d1, *first, *terms1)
        terms0, sums1 = rest[:3], rest[3:]

        def k5(*refs):
            place = Place()
            place.greet()
            jobs = scatters(place, refs[:3], refs[3:6], refs[6:])
            for job in jobs:
                job.begin()
            for event in scatter_events(jobs):
                event()

        sums0 = call(k5, shards, scatter_scratch, 4, *terms0)
        return (d0[None], *(jnp.stack(pair) for pair in zip(sums0, sums1)))

    tokens, rows, out = P(("rep", "dp")), P(None, "dp"), P("rep", "dp")
    return jax.shard_map(
        step, mesh=mesh, in_specs=(tokens, tokens, rows, rows, rows), out_specs=(tokens, out, out, out), check_vma=False
    )
```

```python
import functools

import jax
import jax.numpy as jnp
from jax import lax
from jax.experimental import pallas as pl
from jax.experimental.pallas import tpu as pltpu
from jax.sharding import PartitionSpec as P

BF16, F32 = jnp.bfloat16, jnp.float32
ANY = pl.BlockSpec(memory_space=pl.ANY)
VMEM_LIMIT = 66_500_000
NY, NZ = 2, 4
TOKENS, TILE, CHUNK, RING = 512, 1024, 256, 4


def device(y, z, c):
    return (y * NZ + z) * 2 + c


class Place:
    def __init__(self):
        self.me, self.x = lax.axis_index("dp"), lax.axis_index("rep")
        self.c = lax.rem(self.me, 2)
        self.z = lax.rem(lax.div(self.me, 2), NZ)
        self.y = lax.div(self.me, 2 * NZ)
        self.y_mate = device(1 - self.y, self.z, self.c)
        self.sibling = device(self.y, self.z, 1 - self.c)

    def ahead(self, d):
        return lax.rem(self.z + d, NZ)

    def behind(self, d):
        return lax.rem(self.z + NZ - d, NZ)

    def z_mate(self, d):
        return device(self.y, self.ahead(d), self.c)

    def greet(self, across):
        barrier = pltpu.get_barrier_semaphore()
        mates = [{"dp": self.z_mate(d)} for d in (1, 2, 3)] + [{"dp": self.y_mate}, {"dp": self.sibling}]
        if across:
            mates.append({"rep": 1 - self.x})
        for mate in mates:
            pl.semaphore_signal(barrier, inc=1, device_id=mate, device_id_type=pl.DeviceIdType.MESH)
        pl.semaphore_wait(barrier, len(mates))


def remote(src, dst, send, recv, to):
    return pltpu.make_async_remote_copy(
        src_ref=src, dst_ref=dst, send_sem=send, recv_sem=recv, device_id=to if isinstance(to, dict) else {"dp": to}, device_id_type=pl.DeviceIdType.MESH
    )


class Gather:
    def __init__(self, place, src, out, stage, send, recv, local):
        self.p, self.src, self.out, self.stage, self.send, self.recv, self.local = place, src, out, stage, send, recv, local
        self.rows, self.columns = src.shape
        self.across = {"rep": 1 - place.x}

    def block(self, j):
        return self.out.at[pl.ds(pl.multiple_of(j * self.rows, 8), self.rows), :]

    def half(self, ref, first, x):
        if self.columns % 512 == 0:
            size = self.columns // 2
            return ref.at[pl.ds(pl.multiple_of(first, 8), self.rows), pl.ds(pl.multiple_of(x * size, size), size)]
        size = self.rows // 2
        return ref.at[pl.ds(pl.multiple_of(first + x * size, 8), size), :]

    def part(self, j, x):
        return self.half(self.out, j * self.rows, x)

    def copy(self, src, dst, slot, to):
        return remote(src, dst, self.send.at[slot], self.recv.at[slot], to)

    def begin(self):
        p, mine = self.p, self.block(self.p.me)
        for d in (1, 2, 3):
            if d == 1:
                self.copy(self.src, mine, 0, p.z_mate(d)).start()
            else:
                self.copy(self.half(self.src, 0, p.x), self.part(p.me, p.x), d - 1, p.z_mate(d)).start()
        self.copy(self.src, mine, 3, p.y_mate).start()
        self.copy(self.src, mine, 13, p.sibling).start()
        pltpu.make_async_copy(self.src, self.stage, self.local.at[0]).start()

    def keep(self):
        pltpu.make_async_copy(self.src, self.stage, self.local.at[0]).wait()
        pltpu.make_async_copy(self.stage, self.block(self.p.me), self.local.at[1]).start()

    def from_z(self, d):
        p = self.p
        j = device(p.y, p.behind(d), p.c)
        block, part = self.block(j), self.part(j, p.x)
        if d == 1:
            self.copy(block, block, 0, p.y_mate).wait_recv()
            self.copy(block, block, 14, p.sibling).start()
        else:
            self.copy(part, part, d - 1, p.y_mate).wait_recv()
            self.copy(part, part, 6 + d, self.across).start()
        self.copy(part, part, 3 + d, p.y_mate).start()

    def from_across(self, d):
        p = self.p
        j = device(p.y, p.behind(d), p.c)
        part = self.part(j, 1 - p.x)
        self.copy(part, part, 6 + d, self.across).wait_recv()
        self.copy(self.block(j), self.block(j), 13 + d, p.sibling).start()

    def from_y(self, d):
        p = self.p
        j = device(1 - p.y, p.behind(d), p.c)
        if d == 0:
            block = self.block(j)
            self.copy(block, block, 3, p.y_mate).wait_recv()
            self.copy(block, block, 17, p.sibling).start()
        else:
            part = self.part(j, p.x)
            self.copy(part, part, 3 + d, p.y_mate).wait_recv()
            self.copy(part, part, 9 + d, self.across).start()

    def from_far(self, d):
        p = self.p
        j = device(1 - p.y, p.behind(d), p.c)
        part = self.part(j, 1 - p.x)
        self.copy(part, part, 9 + d, self.across).wait_recv()
        self.copy(self.block(j), self.block(j), 17 + d, p.sibling).start()

    def finish(self):
        p = self.p
        for k in range(8):
            row = p.y if k < 4 else 1 - p.y
            block = self.block(device(row, p.behind(k % 4), 1 - p.c))
            self.copy(block, block, 13 + k, p.sibling).wait_recv()
        mine, part = self.block(p.me), self.part(p.me, p.x)
        for slot in (n for n in range(21) if n != 7):
            sent = mine if slot in (0, 3) or slot >= 13 else part
            self.copy(sent, sent, slot, p.sibling).wait_send()
        pltpu.make_async_copy(self.stage, mine, self.local.at[1]).wait()

    @staticmethod
    def scratch(shape):
        return [pltpu.VMEM(shape, BF16), pltpu.SemaphoreType.DMA((21,)), pltpu.SemaphoreType.DMA((21,)), pltpu.SemaphoreType.DMA((2,))]


class Scatter:
    def __init__(self, place, src, out, own, sib, from_y, from_z, total, send, recv, local):
        self.p, self.src, self.out, self.total = place, src, out, total
        self.own, self.sib, self.y_slots, self.z_slots = own, sib, from_y, from_z
        self.send, self.recv, self.local = send, recv, local
        self.rows = out.shape[0]

    def block(self, k, c):
        row = 1 - self.p.y if k < 4 else self.p.y
        j = device(row, self.p.ahead(k % 4), c)
        return self.src.at[pl.ds(pl.multiple_of(j * self.rows, 8), self.rows), :]

    def to_sibling(self, k):
        return remote(self.block(k, 1 - self.p.c), self.sib.at[k], self.send.at[k], self.recv.at[k], self.p.sibling)

    def to_y(self, d):
        return remote(self.own.at[d], self.y_slots.at[d], self.send.at[8 + d], self.recv.at[8 + d], self.p.y_mate)

    def to_z(self, d):
        return remote(self.own.at[4 + d], self.z_slots.at[d - 1], self.send.at[11 + d], self.recv.at[11 + d], self.p.z_mate(d))

    def load(self, k):
        return pltpu.make_async_copy(self.block(k, self.p.c), self.own.at[k], self.local.at[k])

    def begin(self):
        for k in (1, 2, 3, 0, 5, 6, 7, 4):
            self.to_sibling(k).start()
            self.load(k).start()

    def add(self, refs, to):
        rows, columns = self.rows, self.own.shape[2]
        if columns % 512 == 0:
            count, at = columns // 256, lambda i: (slice(None), pl.ds(pl.multiple_of(i * 256, 256), 256))
        else:
            count, at = rows // 16, lambda i: (pl.ds(pl.multiple_of(i * 16, 16), 16), slice(None))

        def some(i, carry):
            here = at(i)
            value = refs[0][here].astype(F32)
            for ref in refs[1:]:
                value = value + ref[here].astype(F32)
            to[here] = value.astype(BF16)
            return carry

        lax.fori_loop(0, count, some, 0)

    def send_y(self, d):
        self.load(d).wait()
        self.to_sibling(d).wait_recv()
        self.add((self.own.at[d], self.sib.at[d]), self.own.at[d])
        self.to_y(d).start()

    def send_z(self, d):
        self.load(4 + d).wait()
        self.to_sibling(4 + d).wait_recv()
        self.to_y(d).wait_recv()
        self.add((self.own.at[4 + d], self.sib.at[4 + d], self.y_slots.at[d]), self.own.at[4 + d])
        self.to_z(d).start()

    def finish(self):
        self.load(4).wait()
        self.to_sibling(4).wait_recv()
        self.to_y(0).wait_recv()
        for d in (1, 2, 3):
            self.to_z(d).wait_recv()
        self.add([self.own.at[4], self.sib.at[4], self.y_slots.at[0]] + [self.z_slots.at[d] for d in range(3)], self.total)
        store = pltpu.make_async_copy(self.total, self.out, self.local.at[8])
        store.start()
        for k in range(8):
            self.to_sibling(k).wait_send()
        for d in range(4):
            self.to_y(d).wait_send()
        for d in (1, 2, 3):
            self.to_z(d).wait_send()
        store.wait()

    @staticmethod
    def scratch(shape):
        return [pltpu.VMEM((n, *shape), BF16) for n in (8, 8, 4, 3)] + [
            pltpu.VMEM(shape, BF16),
            pltpu.SemaphoreType.DMA((15,)),
            pltpu.SemaphoreType.DMA((15,)),
            pltpu.SemaphoreType.DMA((9,)),
        ]


class Stream:
    def __init__(self, place, outs, own, sib, from_y, from_z, total, send, recv, local):
        self.p, self.outs, self.total = place, outs, total
        self.own, self.sib, self.y_slots, self.z_slots = own, sib, from_y, from_z
        self.send, self.recv, self.local = send, recv, local
        self.rows, self.width = own.shape[5:]

    def mine(self, f, y):
        return self.own.at[lax.rem(f, RING), self.p.c, y]

    def copy(self, f, src, dst, slot, to):
        return remote(src, dst, self.send.at[f, slot], self.recv.at[f, slot], to)

    def to_sibling(self, f):
        return self.copy(f, self.own.at[lax.rem(f, RING), 1 - self.p.c], self.sib.at[f], 0, self.p.sibling)

    def to_y(self, f):
        return self.copy(f, self.mine(f, 1 - self.p.y), self.y_slots.at[f], 1, self.p.y_mate)

    def to_z(self, f, d):
        src = self.mine(f, self.p.y).at[self.p.ahead(d)]
        return self.copy(f, src, self.z_slots.at[f, d - 1], 1 + d, self.p.z_mate(d))

    def store(self, w, f, value):
        slot = lax.rem(f, RING)
        for j in range(16):
            y, z, c = j // 8, j // 2 % 4, j % 2
            self.own[slot, c, y, z, w] = value[j * self.rows : (j + 1) * self.rows].astype(BF16)

    def add(self, refs, to):
        for w in range(2):
            value = refs[0][w].astype(F32)
            for ref in refs[1:]:
                value = value + ref[w].astype(F32)
            to[w] = value.astype(BF16)

    def begin(self, f):
        self.to_sibling(f).start()

    def send_y(self, f):
        self.to_sibling(f).wait_recv()
        mine, sib = self.mine(f, 1 - self.p.y), self.sib.at[f, 1 - self.p.y]
        for z in range(NZ):
            self.add((mine.at[z], sib.at[z]), mine.at[z])
        self.to_y(f).start()

    def send_z(self, f):
        self.to_y(f).wait_recv()
        mine, sib, from_y = self.mine(f, self.p.y), self.sib.at[f, self.p.y], self.y_slots.at[f]
        for d in (1, 2, 3):
            z = self.p.ahead(d)
            self.add((mine.at[z], sib.at[z], from_y.at[z]), mine.at[z])
            self.to_z(f, d).start()

    def result(self, w, f):
        columns = pl.ds(pl.multiple_of(f * self.width, self.width), self.width)
        return pltpu.make_async_copy(self.total.at[f, w], self.outs[w].at[:, columns], self.local.at[f, w])

    def finish(self, f):
        for d in (1, 2, 3):
            self.to_z(f, d).wait_recv()
        terms = [t.at[self.p.z] for t in (self.mine(f, self.p.y), self.sib.at[f, self.p.y], self.y_slots.at[f])]
        self.add(terms + [self.z_slots.at[f, d] for d in range(3)], self.total.at[f])
        for w in range(2):
            self.result(w, f).start()
        self.to_sibling(f).wait_send()
        self.to_y(f).wait_send()
        for d in (1, 2, 3):
            self.to_z(f, d).wait_send()

    def close(self, runs):
        for f in range(runs):
            for w in range(2):
                self.result(w, f).wait()

    @staticmethod
    def scratch(shape):
        rows, columns = shape
        runs, block = columns // CHUNK, (2, rows, CHUNK)
        return [
            pltpu.VMEM((RING, 2, NY, NZ, *block), BF16),
            pltpu.VMEM((runs, NY, NZ, *block), BF16),
            pltpu.VMEM((runs, NZ, *block), BF16),
            pltpu.VMEM((runs, NZ - 1, *block), BF16),
            pltpu.VMEM((runs, *block), BF16),
            pltpu.SemaphoreType.DMA((runs, 5)),
            pltpu.SemaphoreType.DMA((runs, 5)),
            pltpu.SemaphoreType.DMA((runs, 2)),
        ]


def gather_events(jobs, first):
    rounds = []
    for n in range(len(jobs) + 2):
        events = []
        if n < len(jobs):
            events += [functools.partial(jobs[n].from_z, d) for d in (1, 2, 3)]
        if 0 < n <= len(jobs):
            for d in (0, 1, 2, 3):
                if d > 1:
                    events.append(functools.partial(jobs[n - 1].from_across, d))
                events.append(functools.partial(jobs[n - 1].from_y, d))
        if n > 1:
            events += [functools.partial(jobs[n - 2].from_far, d) for d in (1, 2, 3)]
        rounds.append(events)
    before, after = sum(rounds[: first + 2], []), sum(rounds[first + 2 :], [])
    return before + [job.finish for job in jobs[:first]], after + [job.finish for job in jobs[first:]]


def spread(events, steps):
    by_step = [[] for _ in range(steps)]
    for n, event in enumerate(events):
        by_step[n * steps // len(events)].append(event)
    return by_step


def at_step(by_step, step):
    for n, events in enumerate(by_step):
        if events:

            @pl.when(step == n)
            def _(events=events):
                for event in events:
                    event()


def dot(a, b, contract):
    return lax.dot_general(a, b, (contract, ((), ())), preferred_element_type=F32)


def scale_of(wide):
    return lax.rsqrt(jnp.mean(wide * wide, -1, keepdims=True) + 1e-6)


def forward(h, wg, wu, wd, out, hid, a, acc, hook):
    tokens, dim = h.shape
    width = 512
    tiles, chunks = tokens // TOKENS, wg.shape[1] // width

    def body(h, wg, wu, wd, out, hid):
        t, f = pl.program_id(0), pl.program_id(1)
        hook(t * chunks + f)

        @pl.when(f == 0)
        def _():
            wide = h[...].astype(F32)
            a[...] = (wide * scale_of(wide)).astype(BF16)
            acc[...] = jnp.zeros_like(acc)

        gate = dot(a[...], wg[...], ((1,), (0,)))
        up = dot(a[...], wu[...], ((1,), (0,)))
        hid[...] = (gate * jax.nn.sigmoid(gate) * up).astype(BF16)
        acc[...] += dot(hid[...], wd[...], ((1,), (0,)))

        @pl.when(f == chunks - 1)
        def _():
            out[...] = (h[...].astype(F32) + acc[...].astype(BF16).astype(F32)).astype(BF16)

    whole = pl.BlockSpec((TOKENS, dim), lambda t, f: (t, 0))
    pltpu.emit_pipeline(
        body,
        grid=(tiles, chunks),
        in_specs=[
            whole,
            pl.BlockSpec((dim, width), lambda t, f: (0, f)),
            pl.BlockSpec((dim, width), lambda t, f: (0, f)),
            pl.BlockSpec((width, dim), lambda t, f: (f, 0)),
        ],
        out_specs=[whole, pl.BlockSpec((TOKENS, width), lambda t, f: (t, f))],
    )(h, wg, wu, wd, out, hid)


class Layer:
    def __init__(self, h, dy, wg, wu, wd, dh, a, a_t, h_held, dy_held, acc, dgate, dup, hid, local):
        self.h, self.dy, self.wg, self.wu, self.wd, self.dh = h, dy, wg, wu, wd, dh
        self.a, self.a_t, self.h_held, self.dy_held, self.acc = a, a_t, h_held, dy_held, acc
        self.dgate, self.dup, self.hid, self.local = dgate, dup, hid, local
        self.runs = wg.shape[1] // CHUNK

    def tiles(self):
        return [pl.ds(t * TILE, TILE) for t in range(self.h.shape[0] // TILE)]

    def load(self):
        for n, (src, dst) in enumerate(((self.h, self.h_held), (self.dy, self.dy_held))):
            pltpu.make_async_copy(src, dst, self.local.at[n]).start()

    def wait(self, n):
        src, dst = ((self.h, self.h_held), (self.dy, self.dy_held))[n]
        pltpu.make_async_copy(src, dst, self.local.at[n]).wait()

    def norm(self):
        for rows in self.tiles():
            wide = self.h_held[rows].astype(F32)
            a = (wide * scale_of(wide)).astype(BF16)
            self.a[rows] = a
            self.a_t[:, rows] = a.T
            self.acc[rows] = jnp.zeros((TILE, self.acc.shape[1]), F32)

    def loop(self, stream, hook, dwd):
        def body(wg, wu, wd, *down):
            f = pl.program_id(0)
            hook(f)
            for rows in self.tiles():
                a = self.a[rows]
                gate = dot(a, wg[...], ((1,), (0,)))
                up = dot(a, wu[...], ((1,), (0,)))
                dhid = dot(self.dy_held[rows], wd[...], ((1,), (1,))).astype(BF16).astype(F32)
                s = jax.nn.sigmoid(gate)
                silu = gate * s
                if down:
                    self.hid[rows] = (silu * up).astype(BF16)
                by_gate = (dhid * up * (s * (1 + gate * (1 - s)))).astype(BF16)
                by_up = (dhid * silu).astype(BF16)
                self.dgate[rows] = by_gate
                self.dup[rows] = by_up
                self.acc[rows] += dot(by_gate, wg[...], ((1,), (1,))) + dot(by_up, wu[...], ((1,), (1,)))
            stream.store(0, f, dot(self.a_t[...], self.dgate[...], ((1,), (0,))))
            stream.store(1, f, dot(self.a_t[...], self.dup[...], ((1,), (0,))))
            if down:
                down[0][...] = dot(self.hid[...], self.dy_held[...], ((0,), (0,))).astype(BF16)

        dim = self.wg.shape[0]
        wide = pl.BlockSpec((dim, CHUNK), lambda f: (0, f))
        tall = pl.BlockSpec((CHUNK, dim), lambda f: (f, 0))
        pltpu.emit_pipeline(
            body, grid=(self.runs,), in_specs=[wide, wide, tall], out_specs=[tall] * len(dwd)
        )(self.wg, self.wu, self.wd, *dwd)

    def to_dh(self, rows, t):
        return pltpu.make_async_copy(self.h_held.at[rows], self.dh.at[rows], self.local.at[2 + t])

    def by_h(self):
        for t, rows in enumerate(self.tiles()):
            wide = self.h_held[rows].astype(F32)
            scale = scale_of(wide)
            da = self.acc[rows].astype(BF16).astype(F32)
            along = jnp.mean(da * wide, -1, keepdims=True)
            by_h = (da * scale - wide * (along * scale * scale * scale)).astype(BF16)
            self.h_held[rows] = (self.dy_held[rows].astype(F32) + by_h.astype(F32)).astype(BF16)
            self.to_dh(rows, t).start()

    def close(self):
        for t, rows in enumerate(self.tiles()):
            self.to_dh(rows, t).wait()

    @staticmethod
    def scratch(tokens, dim, keeps_hid):
        return (
            [pltpu.VMEM((tokens, dim), BF16), pltpu.VMEM((dim, tokens), BF16)]
            + [pltpu.VMEM((tokens, dim), BF16)] * 2
            + [pltpu.VMEM((tokens, dim), F32)]
            + [pltpu.VMEM((tokens, CHUNK), BF16)] * 2
            + [pltpu.VMEM((tokens if keeps_hid else 16, CHUNK), BF16)]
            + [pltpu.SemaphoreType.DMA((2 + tokens // TILE,))]
        )


def streamed(stream, others):
    def hook(f):
        def earlier(n, step):
            @pl.when(f >= n)
            def _():
                step(f - n)

        earlier(1, stream.begin)
        earlier(3, stream.send_z)
        earlier(2, stream.send_y)
        earlier(4, stream.finish)
        at_step(others, f)

    return hook


def drained(stream, runs, meanwhile):
    last = runs - 1
    stream.begin(last)
    stream.send_y(last - 1)
    stream.send_z(last - 2)
    stream.send_y(last)
    meanwhile()
    stream.finish(last - 3)
    stream.send_z(last - 1)
    stream.finish(last - 2)
    stream.send_z(last)
    stream.finish(last - 1)
    stream.finish(last)
    stream.close(runs)


def by_down(hid, dy, dwd, hook):
    tokens, dim = dy.shape

    def body(hid, dwd):
        hook(pl.program_id(0))
        dwd[...] = dot(hid[...], dy[...], ((0,), (0,))).astype(BF16)

    pltpu.emit_pipeline(
        body,
        grid=(hid.shape[1] // CHUNK,),
        in_specs=[pl.BlockSpec((tokens, CHUNK), lambda f: (0, f))],
        out_specs=[pl.BlockSpec((CHUNK, dim), lambda f: (f, 0))],
    )(hid, dwd)


def call(body, outs, scratch, collective, *args):
    return pl.pallas_call(
        body,
        out_shape=[jax.ShapeDtypeStruct(shape, BF16) for shape in outs],
        in_specs=[ANY] * len(args),
        out_specs=[ANY] * len(outs),
        scratch_shapes=scratch,
        compiler_params=pltpu.CompilerParams(collective_id=collective, has_side_effects=True, vmem_limit_bytes=VMEM_LIMIT),
    )(*args)


def solution(mesh):
    def step(x, dy, *weights):
        tokens, dim = x.shape[1:]
        ff = weights[0].shape[2]
        x, dy = x[0], dy[0]
        shards = [w.shape[1:] for w in weights]
        wholes = [(16 * r, c) for r, c in shards]
        runs = ff // CHUNK
        n_gather = len(Gather.scratch((8, 128)))
        gather_scratch = [s for shape in shards * 2 for s in Gather.scratch(shape)]
        stream_scratch, layer_scratch = Stream.scratch(shards[0]), Layer.scratch(tokens, dim, True)
        down_scratch = Scatter.scratch(shards[2])
        n_stream, n_layer, n_down = len(stream_scratch), len(layer_scratch), len(down_scratch)

        def gather_forward(*refs):
            h, srcs = refs[0], refs[1:4]
            out, hid, wholes = refs[4], refs[5], refs[6:12]
            a, acc, scratch = refs[12], refs[13], refs[14:]
            place = Place()
            place.greet(True)
            jobs = [
                Gather(place, srcs[i % 3].at[i // 3], wholes[i], *scratch[n_gather * i : n_gather * (i + 1)]) for i in range(6)
            ]
            for job in jobs:
                job.begin()
            for job in jobs:
                job.keep()
            before, events = gather_events(jobs, 3)
            for event in before:
                event()
            early = len(events) * 3 // 5
            steps = (tokens // TOKENS) * (ff // 512)
            forward(h, *wholes[:3], out, hid, a, acc, functools.partial(at_step, spread(events[:early], steps)))
            for event in events[early:]:
                event()

        tile = [pltpu.VMEM((TOKENS, dim), BF16), pltpu.VMEM((TOKENS, dim), F32)]
        h1, hid0, *gathered = call(gather_forward, [(tokens, dim), (tokens, ff), *wholes, *wholes], tile + gather_scratch, 1, x, *weights)
        first, second = gathered[:3], gathered[3:]

        def last_layer(*refs):
            dh, dwd, *sums = refs[5:9]
            layer = Layer(*refs[:5], dh, *refs[9 : 9 + n_layer])
            place = Place()
            place.greet(False)
            stream = Stream(place, sums, *refs[9 + n_layer :])
            layer.load()
            layer.wait(0)
            layer.norm()
            layer.wait(1)
            layer.loop(stream, streamed(stream, []), [dwd])
            drained(stream, runs, layer.by_h)
            layer.close()

        d1, down1, *sums1 = call(
            last_layer, [(tokens, dim), wholes[2], *shards[:2]], layer_scratch + stream_scratch, 2, h1, dy, *second
        )

        def first_layer(*refs):
            hid0, down1 = refs[5:7]
            dh, down0, *sums = refs[7:11]
            sum_down0, sum_down1 = refs[11:13]
            scratch = refs[13:]
            layer = Layer(*refs[:5], dh, *scratch[:n_layer])
            place = Place()
            place.greet(False)
            scratch = scratch[n_layer:]
            stream = Stream(place, sums, *scratch[:n_stream])
            scratch = scratch[n_stream:]
            one = Scatter(place, down1, sum_down1, *scratch[:n_down])
            nought = Scatter(place, down0, sum_down0, *scratch[n_down:])
            layer.load()
            one.begin()
            layer.wait(0)
            layer.norm()
            layer.wait(1)
            sends = {2 + n: [functools.partial(one.send_y, d)] for n, d in enumerate((1, 2, 3, 0))}
            by_down(hid0, layer.dy_held, down0, functools.partial(at_step, [sends.get(n, []) for n in range(runs)]))
            nought.begin()
            others = [
                [functools.partial(one.send_z, 1)],
                [functools.partial(one.send_z, 2), functools.partial(one.send_z, 3), functools.partial(nought.send_y, 1)],
                [functools.partial(nought.send_y, 2)],
                [one.finish, functools.partial(nought.send_z, 1)],
                [functools.partial(nought.send_y, 3), functools.partial(nought.send_z, 2)],
                [functools.partial(nought.send_y, 0)],
                [functools.partial(nought.send_z, 3)],
                [],
                [nought.finish],
            ]
            layer.loop(stream, streamed(stream, others), [])
            drained(stream, runs, layer.by_h)
            layer.close()

        d0, _, *rest = call(
            first_layer,
            [(tokens, dim), wholes[2], *shards[:2], shards[2], shards[2]],
            Layer.scratch(tokens, dim, False) + stream_scratch + down_scratch * 2,
            3,
            x,
            d1,
            *first,
            hid0,
            down1,
        )
        sums0 = rest[:3]
        sums1 = [*sums1, rest[3]]
        return (d0[None], *(jnp.stack(pair) for pair in zip(sums0, sums1)))

    tokens, rows, out = P(("rep", "dp")), P(None, "dp"), P("rep", "dp")
    return jax.shard_map(
        step, mesh=mesh, in_specs=(tokens, tokens, rows, rows, rows), out_specs=(tokens, out, out, out), check_vma=False
    )
```

```python
import functools

import jax
import jax.numpy as jnp
from jax import lax
from jax.experimental import pallas as pl
from jax.experimental.pallas import tpu as pltpu
from jax.sharding import PartitionSpec as P

BF16, F32 = jnp.bfloat16, jnp.float32
ANY = pl.BlockSpec(memory_space=pl.ANY)
VMEM_LIMIT = 66_500_000
NY, NZ = 2, 4
PASS = 256
TOKENS, TILE, CHUNK, RING, AHEAD = 512, 1024, 256, 4, 2


def device(y, z, c):
    return (y * NZ + z) * 2 + c


class Place:
    def __init__(self):
        self.me, self.x = lax.axis_index("dp"), lax.axis_index("rep")
        self.c = lax.rem(self.me, 2)
        self.z = lax.rem(lax.div(self.me, 2), NZ)
        self.y = lax.div(self.me, 2 * NZ)
        self.y_mate = device(1 - self.y, self.z, self.c)
        self.sibling = device(self.y, self.z, 1 - self.c)

    def ahead(self, d):
        return lax.rem(self.z + d, NZ)

    def behind(self, d):
        return lax.rem(self.z + NZ - d, NZ)

    def z_mate(self, d):
        return device(self.y, self.ahead(d), self.c)

    def greet(self, across):
        barrier = pltpu.get_barrier_semaphore()
        mates = [{"dp": self.z_mate(d)} for d in (1, 2, 3)] + [{"dp": self.y_mate}, {"dp": self.sibling}]
        if across:
            mates.append({"rep": 1 - self.x})
        for mate in mates:
            pl.semaphore_signal(barrier, inc=1, device_id=mate, device_id_type=pl.DeviceIdType.MESH)
        pl.semaphore_wait(barrier, len(mates))


def remote(src, dst, send, recv, to):
    return pltpu.make_async_remote_copy(
        src_ref=src, dst_ref=dst, send_sem=send, recv_sem=recv, device_id=to if isinstance(to, dict) else {"dp": to}, device_id_type=pl.DeviceIdType.MESH
    )


class Gather:
    def __init__(self, place, src, out, stage, send, recv, local):
        self.p, self.src, self.out, self.stage, self.send, self.recv, self.local = place, src, out, stage, send, recv, local
        self.rows, self.columns = src.shape
        self.across = {"rep": 1 - place.x}

    def block(self, j):
        return self.out.at[pl.ds(pl.multiple_of(j * self.rows, 8), self.rows), :]

    def half(self, ref, first, x):
        if self.columns % 512 == 0:
            size = self.columns // 2
            return ref.at[pl.ds(pl.multiple_of(first, 8), self.rows), pl.ds(pl.multiple_of(x * size, size), size)]
        size = self.rows // 2
        return ref.at[pl.ds(pl.multiple_of(first + x * size, 8), size), :]

    def part(self, j, x):
        return self.half(self.out, j * self.rows, x)

    def copy(self, src, dst, slot, to):
        return remote(src, dst, self.send.at[slot], self.recv.at[slot], to)

    def begin(self):
        p, mine = self.p, self.block(self.p.me)
        for d in (1, 2, 3):
            if d == 1:
                self.copy(self.src, mine, 0, p.z_mate(d)).start()
            else:
                self.copy(self.half(self.src, 0, p.x), self.part(p.me, p.x), d - 1, p.z_mate(d)).start()
        self.copy(self.src, mine, 3, p.y_mate).start()
        self.copy(self.src, mine, 13, p.sibling).start()

    def load(self):
        pltpu.make_async_copy(self.src, self.stage, self.local.at[0]).start()

    def keep(self):
        pltpu.make_async_copy(self.src, self.stage, self.local.at[0]).wait()
        pltpu.make_async_copy(self.stage, self.block(self.p.me), self.local.at[1]).start()

    def from_z(self, d):
        p = self.p
        j = device(p.y, p.behind(d), p.c)
        block, part = self.block(j), self.part(j, p.x)
        if d == 1:
            self.copy(block, block, 0, p.y_mate).wait_recv()
            self.copy(block, block, 14, p.sibling).start()
        else:
            self.copy(part, part, d - 1, p.y_mate).wait_recv()
            self.copy(part, part, 6 + d, self.across).start()
        self.copy(part, part, 3 + d, p.y_mate).start()

    def from_across(self, d):
        p = self.p
        j = device(p.y, p.behind(d), p.c)
        part = self.part(j, 1 - p.x)
        self.copy(part, part, 6 + d, self.across).wait_recv()
        self.copy(self.block(j), self.block(j), 13 + d, p.sibling).start()

    def from_y(self, d):
        p = self.p
        j = device(1 - p.y, p.behind(d), p.c)
        if d == 0:
            block = self.block(j)
            self.copy(block, block, 3, p.y_mate).wait_recv()
            self.copy(block, block, 17, p.sibling).start()
        else:
            part = self.part(j, p.x)
            self.copy(part, part, 3 + d, p.y_mate).wait_recv()
            self.copy(part, part, 9 + d, self.across).start()

    def from_far(self, d):
        p = self.p
        j = device(1 - p.y, p.behind(d), p.c)
        part = self.part(j, 1 - p.x)
        self.copy(part, part, 9 + d, self.across).wait_recv()
        self.copy(self.block(j), self.block(j), 17 + d, p.sibling).start()

    def finish(self):
        p = self.p
        for k in range(8):
            row = p.y if k < 4 else 1 - p.y
            block = self.block(device(row, p.behind(k % 4), 1 - p.c))
            self.copy(block, block, 13 + k, p.sibling).wait_recv()
        mine, part = self.block(p.me), self.part(p.me, p.x)
        for slot in (n for n in range(21) if n != 7):
            sent = mine if slot in (0, 3) or slot >= 13 else part
            self.copy(sent, sent, slot, p.sibling).wait_send()
        pltpu.make_async_copy(self.stage, mine, self.local.at[1]).wait()

    @staticmethod
    def scratch(shape):
        return [pltpu.VMEM(shape, BF16), pltpu.SemaphoreType.DMA((21,)), pltpu.SemaphoreType.DMA((21,)), pltpu.SemaphoreType.DMA((2,))]


class Scatter:
    def __init__(self, place, src, out, own, sib, from_y, from_z, total, send, recv, local):
        self.p, self.src, self.out, self.total = place, src, out, total
        self.own, self.sib, self.y_slots, self.z_slots = own, sib, from_y, from_z
        self.send, self.recv, self.local = send, recv, local
        self.rows = out.shape[0]

    def block(self, k, c):
        row = 1 - self.p.y if k < 4 else self.p.y
        j = device(row, self.p.ahead(k % 4), c)
        return self.src.at[pl.ds(pl.multiple_of(j * self.rows, 8), self.rows), :]

    def to_sibling(self, k):
        return remote(self.block(k, 1 - self.p.c), self.sib.at[k], self.send.at[k], self.recv.at[k], self.p.sibling)

    def to_y(self, d):
        return remote(self.own.at[d], self.y_slots.at[d], self.send.at[8 + d], self.recv.at[8 + d], self.p.y_mate)

    def to_z(self, d):
        return remote(self.own.at[4 + d], self.z_slots.at[d - 1], self.send.at[11 + d], self.recv.at[11 + d], self.p.z_mate(d))

    def load(self, k):
        return pltpu.make_async_copy(self.block(k, self.p.c), self.own.at[k], self.local.at[k])

    def begin(self):
        for k in (1, 2, 3, 0, 5, 6, 7, 4):
            self.to_sibling(k).start()
            self.load(k).start()

    def add(self, refs, to):
        rows, columns = self.rows, self.own.shape[2]
        if columns % 512 == 0:
            count, at = columns // 256, lambda i: (slice(None), pl.ds(pl.multiple_of(i * 256, 256), 256))
        else:
            count, at = rows // 16, lambda i: (pl.ds(pl.multiple_of(i * 16, 16), 16), slice(None))

        def some(i, carry):
            here = at(i)
            value = refs[0][here].astype(F32)
            for ref in refs[1:]:
                value = value + ref[here].astype(F32)
            to[here] = value.astype(BF16)
            return carry

        lax.fori_loop(0, count, some, 0)

    def send_y(self, d):
        self.load(d).wait()
        self.to_sibling(d).wait_recv()
        self.add((self.own.at[d], self.sib.at[d]), self.own.at[d])
        self.to_y(d).start()

    def send_z(self, d):
        self.load(4 + d).wait()
        self.to_sibling(4 + d).wait_recv()
        self.to_y(d).wait_recv()
        self.add((self.own.at[4 + d], self.sib.at[4 + d], self.y_slots.at[d]), self.own.at[4 + d])
        self.to_z(d).start()

    def finish(self):
        self.load(4).wait()
        self.to_sibling(4).wait_recv()
        self.to_y(0).wait_recv()
        for d in (1, 2, 3):
            self.to_z(d).wait_recv()
        self.add([self.own.at[4], self.sib.at[4], self.y_slots.at[0]] + [self.z_slots.at[d] for d in range(3)], self.total)
        store = pltpu.make_async_copy(self.total, self.out, self.local.at[8])
        store.start()
        for k in range(8):
            self.to_sibling(k).wait_send()
        for d in range(4):
            self.to_y(d).wait_send()
        for d in (1, 2, 3):
            self.to_z(d).wait_send()
        store.wait()

    @staticmethod
    def scratch(shape):
        return [pltpu.VMEM((n, *shape), BF16) for n in (8, 8, 4, 3)] + [
            pltpu.VMEM(shape, BF16),
            pltpu.SemaphoreType.DMA((15,)),
            pltpu.SemaphoreType.DMA((15,)),
            pltpu.SemaphoreType.DMA((9,)),
        ]


class Stream:
    def __init__(self, place, outs, own, sib, from_y, from_z, total, send, recv, local):
        self.p, self.outs, self.total = place, outs, total
        self.own, self.sib, self.y_slots, self.z_slots = own, sib, from_y, from_z
        self.send, self.recv, self.local = send, recv, local
        self.rows, self.width = own.shape[5:]

    def mine(self, f, y):
        return self.own.at[lax.rem(f, RING), self.p.c, y]

    def copy(self, f, src, dst, slot, to):
        return remote(src, dst, self.send.at[f, slot], self.recv.at[f, slot], to)

    def to_sibling(self, f):
        return self.copy(f, self.own.at[lax.rem(f, RING), 1 - self.p.c], self.sib.at[f], 0, self.p.sibling)

    def to_y(self, f):
        return self.copy(f, self.mine(f, 1 - self.p.y), self.y_slots.at[f], 1, self.p.y_mate)

    def to_z(self, f, d):
        src = self.mine(f, self.p.y).at[self.p.ahead(d)]
        return self.copy(f, src, self.z_slots.at[f, d - 1], 1 + d, self.p.z_mate(d))

    def store(self, w, f, value):
        slot = lax.rem(f, RING)
        for j in range(16):
            y, z, c = j // 8, j // 2 % 4, j % 2
            self.own[slot, c, y, z, w] = value[j * self.rows : (j + 1) * self.rows].astype(BF16)

    def add(self, refs, to):
        for w in range(2):
            value = refs[0][w].astype(F32)
            for ref in refs[1:]:
                value = value + ref[w].astype(F32)
            to[w] = value.astype(BF16)

    def begin(self, f):
        self.to_sibling(f).start()

    def send_y(self, f):
        self.to_sibling(f).wait_recv()
        mine, sib = self.mine(f, 1 - self.p.y), self.sib.at[f, 1 - self.p.y]
        for z in range(NZ):
            self.add((mine.at[z], sib.at[z]), mine.at[z])
        self.to_y(f).start()

    def send_z(self, f):
        self.to_y(f).wait_recv()
        mine, sib, from_y = self.mine(f, self.p.y), self.sib.at[f, self.p.y], self.y_slots.at[f]
        for d in (1, 2, 3):
            z = self.p.ahead(d)
            self.add((mine.at[z], sib.at[z], from_y.at[z]), mine.at[z])
            self.to_z(f, d).start()

    def result(self, w, f):
        columns = pl.ds(pl.multiple_of(f * self.width, self.width), self.width)
        return pltpu.make_async_copy(self.total.at[f, w], self.outs[w].at[:, columns], self.local.at[f, w])

    def finish(self, f):
        for d in (1, 2, 3):
            self.to_z(f, d).wait_recv()
        terms = [t.at[self.p.z] for t in (self.mine(f, self.p.y), self.sib.at[f, self.p.y], self.y_slots.at[f])]
        self.add(terms + [self.z_slots.at[f, d] for d in range(3)], self.total.at[f])
        for w in range(2):
            self.result(w, f).start()
        self.to_sibling(f).wait_send()
        self.to_y(f).wait_send()
        for d in (1, 2, 3):
            self.to_z(f, d).wait_send()

    def close(self, runs):
        for f in range(runs):
            for w in range(2):
                self.result(w, f).wait()

    @staticmethod
    def scratch(shape):
        rows, columns = shape
        runs, block = columns // CHUNK, (2, rows, CHUNK)
        return [
            pltpu.VMEM((RING, 2, NY, NZ, *block), BF16),
            pltpu.VMEM((runs, NY, NZ, *block), BF16),
            pltpu.VMEM((runs, NZ, *block), BF16),
            pltpu.VMEM((runs, NZ - 1, *block), BF16),
            pltpu.VMEM((runs, *block), BF16),
            pltpu.SemaphoreType.DMA((runs, 5)),
            pltpu.SemaphoreType.DMA((runs, 5)),
            pltpu.SemaphoreType.DMA((runs, 2)),
        ]


def gather_events(jobs, first):
    rounds = []
    for n in range(len(jobs) + 2):
        events = []
        if n < len(jobs):
            events += [functools.partial(jobs[n].from_z, d) for d in (1, 2, 3)]
        if n + AHEAD < len(jobs):
            events.append(jobs[n + AHEAD].begin)
        if 0 < n <= len(jobs):
            for d in (0, 1, 2, 3):
                if d > 1:
                    events.append(functools.partial(jobs[n - 1].from_across, d))
                events.append(functools.partial(jobs[n - 1].from_y, d))
        if n > 1:
            events += [functools.partial(jobs[n - 2].from_far, d) for d in (1, 2, 3)]
        rounds.append(events)
    before, after = sum(rounds[: first + 2], []), sum(rounds[first + 2 :], [])
    return before + [job.finish for job in jobs[:first]], after + [job.finish for job in jobs[first:]]


def spread(events, steps):
    by_step = [[] for _ in range(steps)]
    for n, event in enumerate(events):
        by_step[n * steps // len(events)].append(event)
    return by_step


def at_step(by_step, step):
    for n, events in enumerate(by_step):
        if events:

            @pl.when(step == n)
            def _(events=events):
                for event in events:
                    event()


def dot(a, b, contract):
    return lax.dot_general(a, b, (contract, ((), ())), preferred_element_type=F32)


def scale_of(wide):
    return lax.rsqrt(jnp.mean(wide * wide, -1, keepdims=True) + 1e-6)


def forward(h, wg, wu, wd, out, hid, a, acc, hook):
    tokens, dim = h.shape
    width = 512
    tiles, chunks = tokens // TOKENS, wg.shape[1] // width

    def body(h, wg, wu, wd, out, hid):
        t, f = pl.program_id(0), pl.program_id(1)
        hook(t * chunks + f)

        @pl.when(f == 0)
        def _():
            wide = h[...].astype(F32)
            a[...] = (wide * scale_of(wide)).astype(BF16)
            acc[...] = jnp.zeros_like(acc)

        gate = dot(a[...], wg[...], ((1,), (0,)))
        up = dot(a[...], wu[...], ((1,), (0,)))
        hid[...] = (gate * jax.nn.sigmoid(gate) * up).astype(BF16)
        acc[...] += dot(hid[...], wd[...], ((1,), (0,)))

        @pl.when(f == chunks - 1)
        def _():
            out[...] = (h[...].astype(F32) + acc[...].astype(BF16).astype(F32)).astype(BF16)

    whole = pl.BlockSpec((TOKENS, dim), lambda t, f: (t, 0))
    pltpu.emit_pipeline(
        body,
        grid=(tiles, chunks),
        in_specs=[
            whole,
            pl.BlockSpec((dim, width), lambda t, f: (0, f)),
            pl.BlockSpec((dim, width), lambda t, f: (0, f)),
            pl.BlockSpec((width, dim), lambda t, f: (f, 0)),
        ],
        out_specs=[whole, pl.BlockSpec((TOKENS, width), lambda t, f: (t, f))],
    )(h, wg, wu, wd, out, hid)


class Layer:
    def __init__(self, h, dy, wg, wu, wd, dh, a, a_t, h_held, dy_held, acc, dgate, dup, hid, local):
        self.h, self.dy, self.wg, self.wu, self.wd, self.dh = h, dy, wg, wu, wd, dh
        self.a, self.a_t, self.h_held, self.dy_held, self.acc = a, a_t, h_held, dy_held, acc
        self.dgate, self.dup, self.hid, self.local = dgate, dup, hid, local
        self.runs = wg.shape[1] // CHUNK

    def tiles(self):
        return [pl.ds(t * TILE, TILE) for t in range(self.h.shape[0] // TILE)]

    def load(self):
        for n, (src, dst) in enumerate(((self.h, self.h_held), (self.dy, self.dy_held))):
            pltpu.make_async_copy(src, dst, self.local.at[n]).start()

    def wait(self, n):
        src, dst = ((self.h, self.h_held), (self.dy, self.dy_held))[n]
        pltpu.make_async_copy(src, dst, self.local.at[n]).wait()

    def norm(self):
        def some(t, carry):
            rows = pl.ds(pl.multiple_of(t * PASS, PASS), PASS)
            wide = self.h_held[rows, :].astype(F32)
            a = (wide * scale_of(wide)).astype(BF16)
            self.a[rows, :] = a
            self.a_t[:, rows] = a.T
            self.acc[rows, :] = jnp.zeros((PASS, self.acc.shape[1]), F32)
            return carry

        lax.fori_loop(0, self.h.shape[0] // PASS, some, 0)

    def loop(self, stream, hook, dwd):
        def body(wg, wu, wd, *down):
            f = pl.program_id(0)
            hook(f)
            for rows in self.tiles():
                a = self.a[rows]
                gate = dot(a, wg[...], ((1,), (0,)))
                up = dot(a, wu[...], ((1,), (0,)))
                dhid = dot(self.dy_held[rows], wd[...], ((1,), (1,))).astype(BF16).astype(F32)
                s = jax.nn.sigmoid(gate)
                silu = gate * s
                if down:
                    self.hid[rows] = (silu * up).astype(BF16)
                by_gate = (dhid * up * (s * (1 + gate * (1 - s)))).astype(BF16)
                by_up = (dhid * silu).astype(BF16)
                self.dgate[rows] = by_gate
                self.dup[rows] = by_up
                self.acc[rows] += dot(by_gate, wg[...], ((1,), (1,))) + dot(by_up, wu[...], ((1,), (1,)))
            stream.store(0, f, dot(self.a_t[...], self.dgate[...], ((1,), (0,))))
            stream.store(1, f, dot(self.a_t[...], self.dup[...], ((1,), (0,))))
            if down:
                down[0][...] = dot(self.hid[...], self.dy_held[...], ((0,), (0,))).astype(BF16)

        dim = self.wg.shape[0]
        wide = pl.BlockSpec((dim, CHUNK), lambda f: (0, f))
        tall = pl.BlockSpec((CHUNK, dim), lambda f: (f, 0))
        pltpu.emit_pipeline(
            body, grid=(self.runs,), in_specs=[wide, wide, tall], out_specs=[tall] * len(dwd)
        )(self.wg, self.wu, self.wd, *dwd)

    def to_dh(self, t):
        rows = pl.ds(pl.multiple_of(t * PASS, PASS), PASS)
        return pltpu.make_async_copy(self.h_held.at[rows, :], self.dh.at[rows, :], self.local.at[2 + t])

    def by_h(self):
        def some(t, carry):
            rows = pl.ds(pl.multiple_of(t * PASS, PASS), PASS)
            wide = self.h_held[rows, :].astype(F32)
            scale = scale_of(wide)
            da = self.acc[rows, :].astype(BF16).astype(F32)
            along = jnp.mean(da * wide, -1, keepdims=True)
            by_h = (da * scale - wide * (along * scale * scale * scale)).astype(BF16)
            self.h_held[rows, :] = (self.dy_held[rows, :].astype(F32) + by_h.astype(F32)).astype(BF16)
            self.to_dh(t).start()
            return carry

        lax.fori_loop(0, self.h.shape[0] // PASS, some, 0)

    def close(self):
        for t in range(self.h.shape[0] // PASS):
            self.to_dh(t).wait()

    @staticmethod
    def scratch(tokens, dim, keeps_hid):
        return (
            [pltpu.VMEM((tokens, dim), BF16), pltpu.VMEM((dim, tokens), BF16)]
            + [pltpu.VMEM((tokens, dim), BF16)] * 2
            + [pltpu.VMEM((tokens, dim), F32)]
            + [pltpu.VMEM((tokens, CHUNK), BF16)] * 2
            + [pltpu.VMEM((tokens if keeps_hid else 16, CHUNK), BF16)]
            + [pltpu.SemaphoreType.DMA((2 + tokens // PASS,))]
        )


def streamed(stream, others):
    def hook(f):
        def earlier(n, step):
            @pl.when(f >= n)
            def _():
                step(f - n)

        earlier(1, stream.begin)
        earlier(3, stream.send_z)
        earlier(2, stream.send_y)
        earlier(4, stream.finish)
        at_step(others, f)

    return hook


def drained(stream, runs, meanwhile):
    last = runs - 1
    stream.begin(last)
    stream.send_y(last - 1)
    stream.send_z(last - 2)
    stream.send_y(last)
    meanwhile()
    stream.finish(last - 3)
    stream.send_z(last - 1)
    stream.finish(last - 2)
    stream.send_z(last)
    stream.finish(last - 1)
    stream.finish(last)
    stream.close(runs)


def by_down(hid, dy, dwd, hook):
    tokens, dim = dy.shape

    def body(hid, dwd):
        hook(pl.program_id(0))
        dwd[...] = dot(hid[...], dy[...], ((0,), (0,))).astype(BF16)

    pltpu.emit_pipeline(
        body,
        grid=(hid.shape[1] // CHUNK,),
        in_specs=[pl.BlockSpec((tokens, CHUNK), lambda f: (0, f))],
        out_specs=[pl.BlockSpec((CHUNK, dim), lambda f: (f, 0))],
    )(hid, dwd)


def call(body, outs, scratch, collective, *args):
    return pl.pallas_call(
        body,
        out_shape=[jax.ShapeDtypeStruct(shape, BF16) for shape in outs],
        in_specs=[ANY] * len(args),
        out_specs=[ANY] * len(outs),
        scratch_shapes=scratch,
        compiler_params=pltpu.CompilerParams(collective_id=collective, has_side_effects=True, vmem_limit_bytes=VMEM_LIMIT),
    )(*args)


def solution(mesh):
    def step(x, dy, *weights):
        tokens, dim = x.shape[1:]
        ff = weights[0].shape[2]
        x, dy = x[0], dy[0]
        shards = [w.shape[1:] for w in weights]
        wholes = [(16 * r, c) for r, c in shards]
        runs = ff // CHUNK
        n_gather = len(Gather.scratch((8, 128)))
        gather_scratch = [s for shape in shards * 2 for s in Gather.scratch(shape)]
        stream_scratch, layer_scratch = Stream.scratch(shards[0]), Layer.scratch(tokens, dim, True)
        down_scratch = Scatter.scratch(shards[2])
        n_stream, n_layer, n_down = len(stream_scratch), len(layer_scratch), len(down_scratch)

        def gather_forward(*refs):
            h, srcs = refs[0], refs[1:4]
            out, hid, wholes = refs[4], refs[5], refs[6:12]
            a, acc, scratch = refs[12], refs[13], refs[14:]
            place = Place()
            place.greet(True)
            jobs = [
                Gather(place, srcs[i % 3].at[i // 3], wholes[i], *scratch[n_gather * i : n_gather * (i + 1)]) for i in range(6)
            ]
            for job in jobs[:AHEAD]:
                job.begin()
            for job in jobs:
                job.load()
            for job in jobs:
                job.keep()
            before, events = gather_events(jobs, 3)
            for event in before:
                event()
            early = len(events) * 4 // 5
            steps = (tokens // TOKENS) * (ff // 512)
            forward(h, *wholes[:3], out, hid, a, acc, functools.partial(at_step, spread(events[:early], steps)))
            for event in events[early:]:
                event()

        tile = [pltpu.VMEM((TOKENS, dim), BF16), pltpu.VMEM((TOKENS, dim), F32)]
        h1, hid0, *gathered = call(gather_forward, [(tokens, dim), (tokens, ff), *wholes, *wholes], tile + gather_scratch, 1, x, *weights)
        first, second = gathered[:3], gathered[3:]

        def last_layer(*refs):
            dh, dwd, *sums = refs[5:9]
            layer = Layer(*refs[:5], dh, *refs[9 : 9 + n_layer])
            place = Place()
            place.greet(False)
            stream = Stream(place, sums, *refs[9 + n_layer :])
            layer.load()
            layer.wait(0)
            layer.norm()
            layer.wait(1)
            layer.loop(stream, streamed(stream, []), [dwd])
            drained(stream, runs, layer.by_h)
            layer.close()

        d1, down1, *sums1 = call(
            last_layer, [(tokens, dim), wholes[2], *shards[:2]], layer_scratch + stream_scratch, 2, h1, dy, *second
        )

        def first_layer(*refs):
            hid0, down1 = refs[5:7]
            dh, down0, *sums = refs[7:11]
            sum_down0, sum_down1 = refs[11:13]
            scratch = refs[13:]
            layer = Layer(*refs[:5], dh, *scratch[:n_layer])
            place = Place()
            place.greet(False)
            scratch = scratch[n_layer:]
            stream = Stream(place, sums, *scratch[:n_stream])
            scratch = scratch[n_stream:]
            one = Scatter(place, down1, sum_down1, *scratch[:n_down])
            nought = Scatter(place, down0, sum_down0, *scratch[n_down:])
            layer.load()
            one.begin()
            layer.wait(0)
            layer.norm()
            layer.wait(1)
            sends = {2 + n: [functools.partial(one.send_y, d)] for n, d in enumerate((1, 2, 3, 0))}
            by_down(hid0, layer.dy_held, down0, functools.partial(at_step, [sends.get(n, []) for n in range(runs)]))
            nought.begin()
            others = [
                [functools.partial(one.send_z, 1)],
                [functools.partial(one.send_z, 2), functools.partial(one.send_z, 3), functools.partial(nought.send_y, 1)],
                [functools.partial(nought.send_y, 2)],
                [one.finish, functools.partial(nought.send_z, 1)],
                [functools.partial(nought.send_y, 3), functools.partial(nought.send_z, 2)],
                [functools.partial(nought.send_y, 0)],
                [functools.partial(nought.send_z, 3)],
                [],
                [nought.finish],
            ]
            layer.loop(stream, streamed(stream, others), [])
            drained(stream, runs, layer.by_h)
            layer.close()

        d0, _, *rest = call(
            first_layer,
            [(tokens, dim), wholes[2], *shards[:2], shards[2], shards[2]],
            Layer.scratch(tokens, dim, False) + stream_scratch + down_scratch * 2,
            3,
            x,
            d1,
            *first,
            hid0,
            down1,
        )
        sums0 = rest[:3]
        sums1 = [*sums1, rest[3]]
        return (d0[None], *(jnp.stack(pair) for pair in zip(sums0, sums1)))

    tokens, rows, out = P(("rep", "dp")), P(None, "dp"), P("rep", "dp")
    return jax.shard_map(
        step, mesh=mesh, in_specs=(tokens, tokens, rows, rows, rows), out_specs=(tokens, out, out, out), check_vma=False
    )
```
